32 devices in a mesh: pop: 8 (over z, x), grp: 4 (over y, core).
Axes of the slice: x: 2, y: 2, z: 4, core: 2. Of those that a mesh axis runs over, the one named last changes fastest.
Arguments:
- noise: bfloat16 [128, 1024, 1024], P(('pop', 'grp')), may hold values from -6 to 6
- ranks: int32 [256], P(('pop', 'grp')), may hold values from 0 to 255, each once
- lengths: int32 [256], P(('pop', 'grp')), may hold values from 1 to 16
- start_state: float32 [32, 256], replicated, may hold values from -6 to 6
- w_first: bfloat16 [256, 1024], replicated, may hold values from -0.375 to 0.375
- w_mid: bfloat16 [1024, 1024], replicated, may hold values from -0.1875 to 0.1875
- w_last: bfloat16 [1024, 64], replicated, may hold values from -0.1875 to 0.1875
- dynamics: float32 [256, 256], replicated, may hold values from -0.25 to 0.25
- control: float32 [64, 256], replicated, may hold values from -0.75 to 0.75
Outputs:
- returns: float32 [256], P(('pop', 'grp'))
- gradient: float32 [1024, 1024], P('pop', 'grp')
The draws below stay inside these ranges and needn't reach their ends.
Inputs may be any that keep to these rules, and one draw needn't show every extreme that they name: `ranks`: each member's rank appears once.
All inputs are finite; a program needn't handle non-finite values.
Results may differ from the reference program's by a relative error of at most 0.0028.
Values may be sent and summed in bfloat16 or wider, within the bound.
No kernel may reach another device: no remote copies, remote signals or barrier semaphores. Data moves between devices by JAX's collectives and lax.ppermute only.
A program may use at most 128 MiB of HBM per device.

```python
import jax
import jax.numpy as jnp
from jax import lax

OBS = 256
HID = 1024
ACT = 64
STEPS = 16
BATCH = 32
NOISE = 128
POP = 256


def with_ends(result, key, smallest, top_value):
    longest = result.shape.index(max(result.shape))
    spots = []
    for shift in (0, 1):
        where = [jax.random.randint(jax.random.fold_in(key, axis), (), 0, length) for axis, length in enumerate(result.shape)]
        where[longest] = (where[longest] + shift) % result.shape[longest]
        spots.append(tuple(where))
    return result.at[spots[0]].set(smallest).at[spots[1]].set(top_value)


def with_spikes(values, stream_key, source, target, shards_of, factor):
    owner, partner = [(jnp.arange(values.shape[position]) // (values.shape[position] // shards_of)).reshape([-1 if axis == position else 1 for axis in range(values.ndim)]) for position in (source, target)]
    chosen = jax.random.permutation(stream_key, shards_of)[partner]
    strong = (owner == chosen) | (owner == (partner + shards_of // 2) % shards_of)
    return jnp.where(strong, factor * values, values)


def level_of(stream_key, extent, cuts, smallest, top_value):
    level = 1.0
    for position, parts in cuts:
        steps = jax.random.uniform(jax.random.fold_in(jax.random.fold_in(stream_key, 6), position), (parts,), jnp.float32, smallest / len(cuts), top_value / len(cuts))
        level = level * jnp.repeat(jnp.exp(steps), extent[position] // parts).reshape((-1,) + (1,) * (len(extent) - 1 - position))
    return level


def gaussian(rng, dims, spread, limit, split=(), held_as=jnp.bfloat16):
    result = jax.random.normal(rng, dims, jnp.float32) * spread
    if len(split) > 0:
        result = level_of(rng, dims, split, -0.22, 0.18) * result
    return jnp.clip(result, min=-limit, max=limit).astype(held_as)


def heavy_noise(rng, dims, deviation, limit, pieces, heavy, kind=jnp.bfloat16):
    drawn = deviation * jax.random.normal(rng, dims, jnp.float32)
    if pieces:
        drawn = drawn * level_of(rng, dims, pieces, -0.22, 0.18)
    return jnp.clip(with_spikes(drawn, jax.random.fold_in(rng, 3), *heavy), -limit, limit).astype(kind)


def setup_inputs(seed: int = 0) -> dict:
    seeds = jax.random.split(jax.random.key(seed), 10)
    noise = heavy_noise(seeds[0], (NOISE, HID, HID), 1.0, 6.0, ((0, 32),), (0, 1, 32, 2.75))
    ranks = jax.random.permutation(seeds[1], POP).astype(jnp.int32)
    lengths = with_ends(jax.random.randint(seeds[2], (POP,), 1, STEPS + 1), jax.random.fold_in(seeds[2], 1), 1, STEPS).astype(jnp.int32)
    start_state = gaussian(seeds[3], (BATCH, OBS), 1.0, 6.0, (), jnp.float32)
    w_first = gaussian(seeds[4], (OBS, HID), OBS ** -0.5, 0.375)
    w_mid = gaussian(seeds[5], (HID, HID), HID ** -0.5, 0.1875)
    w_last = gaussian(seeds[6], (HID, ACT), HID ** -0.5, 0.1875)
    dynamics = gaussian(seeds[7], (OBS, OBS), (2 * OBS) ** -0.5, 0.25, (), jnp.float32)
    control = gaussian(seeds[8], (ACT, OBS), ACT ** -0.5, 0.75, (), jnp.float32)
    return dict(noise=noise, ranks=ranks, lengths=lengths, start_state=start_state, w_first=w_first, w_mid=w_mid, w_last=w_last, dynamics=dynamics, control=control)


noise_scale = 0.02
effort_cost = 0.1


def rollout(member_weight, start_state, w_first, w_last, dynamics, control, length):
    def advance(carried, moment):
        states, totals = carried
        first = jnp.tanh(jnp.dot(states.astype(jnp.bfloat16), w_first, preferred_element_type=jnp.float32)).astype(jnp.bfloat16)
        second = jnp.tanh(jnp.dot(first, member_weight, preferred_element_type=jnp.float32)).astype(jnp.bfloat16)
        action = jnp.tanh(jnp.dot(second, w_last, preferred_element_type=jnp.float32))
        next_state = jnp.dot(states, dynamics, precision=lax.Precision.HIGHEST) + jnp.dot(action, control, precision=lax.Precision.HIGHEST)
        reward = -jnp.mean(next_state * next_state, axis=1) - effort_cost * jnp.mean(action * action, axis=1)
        totals = totals + jnp.where(moment < length, reward, jnp.zeros_like(reward))
        return (next_state, totals), None

    start = (start_state, jnp.zeros((BATCH,), jnp.float32))
    (final_state, totals), _ = lax.scan(advance, start, jnp.arange(STEPS, dtype=jnp.int32))
    return jnp.mean(totals) / STEPS


def reference(noise, ranks, lengths, start_state, w_first, w_mid, w_last, dynamics, control):
    base = w_mid.astype(jnp.float32)

    def rollout_pair(index):
        perturb = noise[index].astype(jnp.float32)
        upward = (base + noise_scale * perturb).astype(jnp.bfloat16)
        downward = (base - noise_scale * perturb).astype(jnp.bfloat16)
        first_return = rollout(upward, start_state, w_first, w_last, dynamics, control, lengths[2 * index])
        second_return = rollout(downward, start_state, w_first, w_last, dynamics, control, lengths[2 * index + 1])
        return jnp.stack([first_return, second_return])

    returns = lax.map(rollout_pair, jnp.arange(NOISE, dtype=jnp.int32)).reshape(POP)
    weights = ranks.astype(jnp.float32) / (POP - 1) - 0.5
    pair_weight = (weights[0::2] - weights[1::2]).astype(jnp.bfloat16)
    flat = noise.reshape(NOISE, HID * HID)
    summed = jnp.dot(pair_weight, flat, preferred_element_type=jnp.float32).reshape(HID, HID)
    gradient = summed / (NOISE * noise_scale)
    return returns, gradient
```

```python
import functools

import jax
import jax.numpy as jnp
from jax import lax
from jax.experimental import pallas as pl
from jax.experimental.pallas import tpu as pltpu
from jax.sharding import PartitionSpec as P

STEPS = 16
CHUNKS = (7, 9)
F32, BF16 = jnp.float32, jnp.bfloat16

noise_scale = 0.02
effort_cost = 0.1


def dot(a, b):
    return jnp.dot(a, b, preferred_element_type=F32)


def partial_kernel(total_pairs, where, ranks, noise, out):
    pair_count = noise.shape[0]
    total = None
    for k in range(pair_count):
        up = jnp.full(noise.shape[1:], ranks[2 * k], jnp.int32).astype(F32) / (2 * total_pairs - 1) - 0.5
        down = jnp.full(noise.shape[1:], ranks[2 * k + 1], jnp.int32).astype(F32) / (2 * total_pairs - 1) - 0.5
        weight = (up - down).astype(BF16).astype(F32)
        term = weight * noise[k].astype(F32)
        total = term if total is None else total + term
    out[...] = total.astype(out.dtype)[None, None, None]


def partial_sum(noise, ranks, where, flip, sizes, total_pairs, dtype):
    pair_count, rows, columns = noise.shape
    nz, nx, ny, nc = sizes
    r, c = rows // (nz * nx), columns // (ny * nc)

    def source(dx, dy, dz, here, ranks):
        x, y, z = lax.rem(here[1] + dx, nx), lax.rem(here[2] + dy, ny), lax.rem(here[0] + dz, nz)
        core = lax.rem(here[3] + flip, nc)
        return (0, z * nx + x, y * nc + core)

    return pl.pallas_call(
        functools.partial(partial_kernel, total_pairs),
        out_shape=jax.ShapeDtypeStruct((nx, ny, nz, r, c), dtype),
        grid_spec=pltpu.PrefetchScalarGridSpec(
            num_scalar_prefetch=2,
            grid=(nx, ny, nz),
            in_specs=[pl.BlockSpec((pair_count, r, c), source)],
            out_specs=pl.BlockSpec((1, 1, 1, r, c), lambda dx, dy, dz, here, ranks: (dx, dy, dz, 0, 0)),
        ),
        compiler_params=pltpu.CompilerParams(vmem_limit_bytes=8 * 2**20),
        cost_estimate=pl.CostEstimate(flops=4 * 10**8, bytes_accessed=noise.size, transcendentals=0),
        name=f"partial_{flip}",
    )(where, ranks, noise)


def rollout_kernel(begin, end, *refs):
    first_call, last_call = begin == 0, end == STEPS
    lengths, w_first, w_mid, noise = refs[:4]
    if first_call:
        start_state, w_last, dynamics, control = refs[4:8]
        rest = refs[8:]
    else:
        states_in, last_in, dynamics_in, control_in, squares_in, efforts_in = refs[4:10]
        rest = refs[10:]
    if last_call:
        returns, states, last, dyn, ctl, squares, efforts = rest
    else:
        states, last, dyn, ctl, squares, efforts = rest
    pair_count, _, hidden = noise.shape
    members = 2 * pair_count
    obs = w_first.shape[0]
    rows = states.shape[0]
    batch = rows // members
    if first_call:
        tall = w_last[...].astype(F32).T
        last[...] = jnp.concatenate([tall, tall], axis=1).astype(BF16)
        whole = dynamics[...]
        high = whole.astype(BF16)
        dyn[0] = high
        dyn[1] = (whole - high.astype(F32)).astype(BF16)
        whole = control[...]
        high = whole.astype(BF16)
        ctl[...] = jnp.concatenate([high, (whole - high.astype(F32)).astype(BF16)], axis=0)
        for m in range(members):
            states[pl.ds(m * batch, batch), :] = start_state[...]
        squares[...] = jnp.zeros_like(squares)
        efforts[...] = jnp.zeros_like(efforts)
    else:
        last[...] = last_in[...]
        dyn[...] = dynamics_in[...]
        ctl[...] = control_in[...]
        states[...] = states_in[...]
        squares[...] = squares_in[...]
        efforts[...] = efforts_in[...]
    row = lax.broadcasted_iota(jnp.int32, (rows, 1), 0)
    scale = jnp.where(lax.rem(row // batch, 2) == 0, noise_scale, -noise_scale).astype(F32)

    def step(moment, carry):
        low = states[...].astype(BF16)
        first = jnp.tanh(dot(low, w_first[...]))
        scaled = (first * scale).astype(BF16)
        shared = dot(first.astype(BF16), w_mid[...])
        own = jnp.concatenate(
            [dot(scaled[p * 2 * batch : (p + 1) * 2 * batch], noise[p]) for p in range(pair_count)], axis=0
        )
        second = jnp.tanh(shared + own).astype(BF16)
        action = jnp.tanh(dot(second, last[...]))
        state = dot(low, dyn[0]) + dot(low, dyn[1]) + dot(action.astype(BF16), ctl[...])
        states[...] = state
        for m in range(members):
            alive = jnp.where(moment < lengths[m], 1.0, 0.0)
            s, a = state[m * batch : (m + 1) * batch], action[m * batch : (m + 1) * batch]
            squares[m] += alive * (s * s).reshape(batch // 8, 8, s.shape[1]).sum(axis=0)
            efforts[m] += alive * (a * a).reshape(batch // 8, 8, a.shape[1]).sum(axis=0)
        return carry

    lax.fori_loop(begin, end, step, 0)
    if last_call:
        acts = efforts.shape[2]
        for m in range(members):
            returns[m] = jnp.sum(squares[m]) * (-1.0 / (obs * batch * STEPS)) + jnp.sum(efforts[m]) * (
                -effort_cost / (acts * batch * STEPS)
            )


def rollout(begin, end, lengths, w_first, w_mid, noise, others):
    pair_count, hidden, _ = noise.shape
    obs = w_first.shape[0]
    members = 2 * pair_count
    if begin == 0:
        start_state, w_last = others[:2]
        batch, acts = start_state.shape[0], w_last.shape[0]
    else:
        batch, acts = others[0].shape[0] // members, others[1].shape[1] // 2
    rows = members * batch
    kept = [
        ((rows, obs), F32),
        ((hidden, 2 * acts), BF16),
        ((2, obs, obs), BF16),
        ((2 * acts, obs), BF16),
        ((members, 8, obs), F32),
        ((members, 8, 2 * acts), F32),
    ]
    vmem, smem = pl.BlockSpec(memory_space=pltpu.VMEM), pl.BlockSpec(memory_space=pltpu.SMEM)
    if end == STEPS:
        out_shape = jax.ShapeDtypeStruct((members,), F32)
        out_specs = smem
        scratch = [pltpu.VMEM(*k) for k in kept]
    else:
        out_shape = [jax.ShapeDtypeStruct(*k) for k in kept]
        out_specs = [vmem] * len(kept)
        scratch = []
    macs = (end - begin) * rows * hidden * (2 * hidden + 2 * obs)
    return pl.pallas_call(
        functools.partial(rollout_kernel, begin, end),
        out_shape=out_shape,
        in_specs=[smem] + [vmem] * (3 + len(others)),
        out_specs=out_specs,
        scratch_shapes=scratch,
        compiler_params=pltpu.CompilerParams(vmem_limit_bytes=32 * 2**20),
        cost_estimate=pl.CostEstimate(flops=2 * macs, bytes_accessed=2 * noise.size, transcendentals=0),
        name=f"rollout_{begin}",
    )(lengths, w_first, w_mid, noise, *others)


def on_device(sizes, noise, ranks, lengths, start_state, w_first, w_mid, w_last, dynamics, control):
    nz, nx, ny, nc = sizes
    total_pairs = noise.shape[0] * nz * nx * ny * nc
    pop, grp = lax.axis_index("pop"), lax.axis_index("grp")
    where = jnp.stack([pop // nx, pop % nx, grp // nc, grp % nc]).astype(jnp.int32)

    def shift(value, dz, dx, dy, dc):
        pairs = []
        for z in range(nz):
            for x in range(nx):
                for y in range(ny):
                    for c in range(nc):
                        tz, tx, ty, tc = (z + dz) % nz, (x + dx) % nx, (y + dy) % ny, (c + dc) % nc
                        pairs.append((((z * nx + x) * ny + y) * nc + c, ((tz * nx + tx) * ny + ty) * nc + tc))
        return lax.ppermute(value, ("pop", "grp"), pairs)

    total = None
    for dc in range(1, nc):
        part = shift(partial_sum(noise, ranks, where, dc, sizes, total_pairs, BF16), 0, 0, 0, dc).astype(F32)
        total = part if total is None else total + part
    total = partial_sum(noise, ranks, where, 0, sizes, total_pairs, F32) + total

    mine = total[0, 0]
    for dx in range(nx):
        for dy in range(ny):
            if dx or dy:
                mine = mine + shift(total[dx, dy].astype(BF16), 0, dx, dy, 0).astype(F32)
    carried = rollout(0, CHUNKS[0], lengths, w_first, w_mid, noise, (start_state, w_last.T, dynamics, control))
    mine, carried = lax.optimization_barrier((mine, carried))
    result = mine[0]
    for dz in range(1, nz):
        result = result + shift(mine[dz].astype(BF16), dz, 0, 0, 0).astype(F32)
    returns = rollout(CHUNKS[0], STEPS, lengths, w_first, w_mid, noise, carried)
    gradient = result / (total_pairs * noise_scale)
    return (returns, gradient)


def solution(mesh):
    pop, grp = mesh.shape["pop"], mesh.shape["grp"]
    nx = max(1, pop // 4)
    nc = 2 if grp % 2 == 0 else 1
    sizes = (pop // nx, nx, grp // nc, nc)
    return jax.shard_map(
        functools.partial(on_device, sizes),
        mesh=mesh,
        in_specs=(
            P(("pop", "grp"), None, None),
            P(("pop", "grp")),
            P(("pop", "grp")),
            P(),
            P(),
            P(),
            P(),
            P(),
            P(),
        ),
        out_specs=(P(("pop", "grp")), P("pop", "grp")),
        check_vma=False,
    )
```

```python
import functools

import jax
import jax.numpy as jnp
from jax import lax
from jax.experimental import pallas as pl
from jax.experimental.pallas import tpu as pltpu
from jax.sharding import PartitionSpec as P

STEPS = 16
CHUNKS = (7, 9)
F32, BF16 = jnp.float32, jnp.bfloat16

noise_scale = 0.02
effort_cost = 0.1


def dot(a, b):
    return jnp.dot(a, b, preferred_element_type=F32)


def pair_weights(rank, pair_count, total_pairs, width):
    weights = []
    for k in range(pair_count):
        up = jnp.full((1, width), rank[2 * k], jnp.int32).astype(F32) / (2 * total_pairs - 1) - 0.5
        down = jnp.full((1, width), rank[2 * k + 1], jnp.int32).astype(F32) / (2 * total_pairs - 1) - 0.5
        weights.append((up - down).astype(BF16).astype(F32))
    return weights


def block_places(sizes, flip, r, c):
    nz, nx, ny, nc = sizes
    pop, grp = lax.axis_index("pop"), lax.axis_index("grp")
    z0, x0, y0, c0 = pop // nx, lax.rem(pop, nx), grp // nc, lax.rem(grp, nc)
    places = []
    for dx in range(nx):
        for dy in range(ny):
            for dz in range(nz):
                row = lax.rem(z0 + dz, nz) * nx + lax.rem(x0 + dx, nx)
                column = lax.rem(y0 + dy, ny) * nc + lax.rem(c0 + flip, nc)
                rows, columns = pl.ds(pl.multiple_of(row * r, r), r), pl.ds(pl.multiple_of(column * c, c), c)
                places.append(((dx, dy, dz), rows, columns))
    return places


def weighted_block(weights, held, rows, columns):
    total = None
    for k, weight in enumerate(weights):
        term = weight * held[k, rows, columns].astype(F32)
        total = term if total is None else total + term
    return total


def load_kernel(sizes, total_pairs, ranks, noise, held, out, rank, sems, rank_sem):
    pair_count = noise.shape[0]
    r, c = out.shape[4:]
    nc = sizes[3]
    copies = []
    ranks_copy = pltpu.make_async_copy(ranks, rank, rank_sem)
    ranks_copy.start()
    for flip in list(range(1, nc)) + [0]:
        for _, rows, columns in block_places(sizes, flip, r, c):
            here = (slice(None), rows, columns)
            copies.append(pltpu.make_async_copy(noise.at[here], held.at[here], sems.at[len(copies)]))
            copies[-1].start()
    ranks_copy.wait()
    weights = pair_weights(rank, pair_count, total_pairs, c)
    n = 0
    for flip in range(1, nc):
        for where, rows, columns in block_places(sizes, flip, r, c):
            copies[n].wait()
            n += 1
            out[(flip - 1,) + where] = weighted_block(weights, held, rows, columns).astype(out.dtype)
    for copy in copies[n:]:
        copy.wait()


def own_kernel(sizes, total_pairs, rank, held, out):
    r, c = out.shape[3:]
    weights = pair_weights(rank, held.shape[0], total_pairs, c)
    for where, rows, columns in block_places(sizes, 0, r, c):
        out[where] = weighted_block(weights, held, rows, columns)


def load_noise(noise, ranks, sizes, total_pairs):
    pair_count, rows, columns = noise.shape
    nz, nx, ny, nc = sizes
    r, c = rows // (nz * nx), columns // (ny * nc)
    hbm, vmem = pl.BlockSpec(memory_space=pltpu.HBM), pl.BlockSpec(memory_space=pltpu.VMEM)
    blocks = nx * ny * nz * nc
    return pl.pallas_call(
        functools.partial(load_kernel, sizes, total_pairs),
        out_shape=(
            jax.ShapeDtypeStruct(noise.shape, BF16),
            jax.ShapeDtypeStruct((nc - 1, nx, ny, nz, r, c), BF16),
        ),
        in_specs=[hbm, hbm],
        out_specs=(vmem, vmem),
        scratch_shapes=[
            pltpu.SMEM(ranks.shape, jnp.int32),
            pltpu.SemaphoreType.DMA((blocks,)),
            pltpu.SemaphoreType.DMA,
        ],
        compiler_params=pltpu.CompilerParams(vmem_limit_bytes=42 * 2**20),
        cost_estimate=pl.CostEstimate(flops=10**8, bytes_accessed=2 * noise.size, transcendentals=0),
        name="load",
    )(ranks, noise)


def own_half(held, ranks, sizes, total_pairs):
    pair_count, rows, columns = held.shape
    nz, nx, ny, nc = sizes
    r, c = rows // (nz * nx), columns // (ny * nc)
    vmem, smem = pl.BlockSpec(memory_space=pltpu.VMEM), pl.BlockSpec(memory_space=pltpu.SMEM)
    return pl.pallas_call(
        functools.partial(own_kernel, sizes, total_pairs),
        out_shape=jax.ShapeDtypeStruct((nx, ny, nz, r, c), F32),
        in_specs=[smem, vmem],
        out_specs=vmem,
        compiler_params=pltpu.CompilerParams(vmem_limit_bytes=32 * 2**20),
        cost_estimate=pl.CostEstimate(flops=10**8, bytes_accessed=held.size, transcendentals=0),
        name="own",
    )(ranks, held)


def rollout_kernel(begin, end, *refs):
    first_call, last_call = begin == 0, end == STEPS
    lengths, w_first, w_mid, noise = refs[:4]
    if first_call:
        start_state, w_last, dynamics, control = refs[4:8]
        rest = refs[8:]
    else:
        states_in, last_in, dynamics_in, control_in, squares_in, efforts_in = refs[4:10]
        rest = refs[10:]
    if last_call:
        returns, states, last, dyn, ctl, squares, efforts = rest
    else:
        states, last, dyn, ctl, squares, efforts = rest
    pair_count, _, hidden = noise.shape
    members = 2 * pair_count
    obs = w_first.shape[0]
    rows = states.shape[0]
    batch = rows // members
    if first_call:
        tall = w_last[...].astype(F32).T
        last[...] = jnp.concatenate([tall, tall], axis=1).astype(BF16)
        whole = dynamics[...]
        high = whole.astype(BF16)
        dyn[0] = high
        dyn[1] = (whole - high.astype(F32)).astype(BF16)
        whole = control[...]
        high = whole.astype(BF16)
        ctl[...] = jnp.concatenate([high, (whole - high.astype(F32)).astype(BF16)], axis=0)
        for m in range(members):
            states[pl.ds(m * batch, batch), :] = start_state[...]
        squares[...] = jnp.zeros_like(squares)
        efforts[...] = jnp.zeros_like(efforts)
    else:
        last[...] = last_in[...]
        dyn[...] = dynamics_in[...]
        ctl[...] = control_in[...]
        states[...] = states_in[...]
        squares[...] = squares_in[...]
        efforts[...] = efforts_in[...]
    row = lax.broadcasted_iota(jnp.int32, (rows, 1), 0)
    scale = jnp.where(lax.rem(row // batch, 2) == 0, noise_scale, -noise_scale).astype(F32)

    def step(moment, carry):
        low = states[...].astype(BF16)
        first = jnp.tanh(dot(low, w_first[...]))
        scaled = (first * scale).astype(BF16)
        shared = dot(first.astype(BF16), w_mid[...])
        own = jnp.concatenate(
            [dot(scaled[p * 2 * batch : (p + 1) * 2 * batch], noise[p]) for p in range(pair_count)], axis=0
        )
        second = jnp.tanh(shared + own).astype(BF16)
        action = jnp.tanh(dot(second, last[...]))
        state = dot(low, dyn[0]) + dot(low, dyn[1]) + dot(action.astype(BF16), ctl[...])
        states[...] = state
        for m in range(members):
            alive = jnp.where(moment < lengths[m], 1.0, 0.0)
            s, a = state[m * batch : (m + 1) * batch], action[m * batch : (m + 1) * batch]
            squares[m] += alive * (s * s).reshape(batch // 8, 8, s.shape[1]).sum(axis=0)
            efforts[m] += alive * (a * a).reshape(batch // 8, 8, a.shape[1]).sum(axis=0)
        return carry

    lax.fori_loop(begin, end, step, 0)
    if last_call:
        acts = efforts.shape[2]
        sums = jnp.sum(squares[...].sum(axis=1), axis=1, keepdims=True) * (-1.0 / (obs * batch * STEPS))
        sums += jnp.sum(efforts[...].sum(axis=1), axis=1, keepdims=True) * (-effort_cost / (acts * batch * STEPS))
        here = lax.broadcasted_iota(jnp.int32, (members, members), 0)
        there = lax.broadcasted_iota(jnp.int32, (members, members), 1)
        returns[...] = jnp.sum(jnp.where(here == there, sums, 0.0), axis=0)


def rollout(begin, end, lengths, w_first, w_mid, noise, others):
    pair_count, hidden, _ = noise.shape
    obs = w_first.shape[0]
    members = 2 * pair_count
    if begin == 0:
        start_state, w_last = others[:2]
        batch, acts = start_state.shape[0], w_last.shape[0]
    else:
        batch, acts = others[0].shape[0] // members, others[1].shape[1] // 2
    rows = members * batch
    kept = [
        ((rows, obs), F32),
        ((hidden, 2 * acts), BF16),
        ((2, obs, obs), BF16),
        ((2 * acts, obs), BF16),
        ((members, 8, obs), F32),
        ((members, 8, 2 * acts), F32),
    ]
    vmem, smem = pl.BlockSpec(memory_space=pltpu.VMEM), pl.BlockSpec(memory_space=pltpu.SMEM)
    if end == STEPS:
        out_shape = jax.ShapeDtypeStruct((members,), F32)
        out_specs = vmem
        scratch = [pltpu.VMEM(*k) for k in kept]
    else:
        out_shape = [jax.ShapeDtypeStruct(*k) for k in kept]
        out_specs = [vmem] * len(kept)
        scratch = []
    macs = (end - begin) * rows * hidden * (2 * hidden + 2 * obs)
    return pl.pallas_call(
        functools.partial(rollout_kernel, begin, end),
        out_shape=out_shape,
        in_specs=[smem] + [vmem] * (3 + len(others)),
        out_specs=out_specs,
        scratch_shapes=scratch,
        compiler_params=pltpu.CompilerParams(vmem_limit_bytes=32 * 2**20),
        cost_estimate=pl.CostEstimate(flops=2 * macs, bytes_accessed=2 * noise.size, transcendentals=0),
        name=f"rollout_{begin}",
    )(lengths, w_first, w_mid, noise, *others)


def on_device(sizes, noise, ranks, lengths, start_state, w_first, w_mid, w_last, dynamics, control):
    nz, nx, ny, nc = sizes
    total_pairs = noise.shape[0] * nz * nx * ny * nc

    def shift(value, dz, dx, dy, dc):
        pairs = []
        for z in range(nz):
            for x in range(nx):
                for y in range(ny):
                    for c in range(nc):
                        tz, tx, ty, tc = (z + dz) % nz, (x + dx) % nx, (y + dy) % ny, (c + dc) % nc
                        pairs.append((((z * nx + x) * ny + y) * nc + c, ((tz * nx + tx) * ny + ty) * nc + tc))
        return lax.ppermute(value, ("pop", "grp"), pairs)

    noise, sent = load_noise(noise, ranks, sizes, total_pairs)
    total = own_half(noise, ranks, sizes, total_pairs)
    for dc in range(1, nc):
        total = total + shift(sent[dc - 1], 0, 0, 0, dc).astype(F32)

    mine = total[0, 0]
    for dx in range(nx):
        for dy in range(ny):
            if dx or dy:
                mine = mine + shift(total[dx, dy].astype(BF16), 0, dx, dy, 0).astype(F32)
    carried = rollout(0, CHUNKS[0], lengths, w_first, w_mid, noise, (start_state, w_last.T, dynamics, control))
    mine, carried = lax.optimization_barrier((mine, carried))
    result = mine[0]
    for dz in range(1, nz):
        result = result + shift(mine[dz], dz, 0, 0, 0)
    returns = rollout(CHUNKS[0], STEPS, lengths, w_first, w_mid, noise, carried)
    gradient = result / (total_pairs * noise_scale)
    return (returns, gradient)


def solution(mesh):
    pop, grp = mesh.shape["pop"], mesh.shape["grp"]
    nx = max(1, pop // 4)
    nc = 2 if grp % 2 == 0 else 1
    sizes = (pop // nx, nx, grp // nc, nc)
    return jax.shard_map(
        functools.partial(on_device, sizes),
        mesh=mesh,
        in_specs=(
            P(("pop", "grp"), None, None),
            P(("pop", "grp")),
            P(("pop", "grp")),
            P(),
            P(),
            P(),
            P(),
            P(),
            P(),
        ),
        out_specs=(P(("pop", "grp")), P("pop", "grp")),
        check_vma=False,
    )
```

```python
import functools

import jax
import jax.numpy as jnp
from jax import lax
from jax.experimental import pallas as pl
from jax.experimental.pallas import tpu as pltpu
from jax.sharding import PartitionSpec as P

STEPS = 16
CUTS = (0, 1, 8, STEPS)
F32, BF16 = jnp.float32, jnp.bfloat16

noise_scale = 0.02
effort_cost = 0.1


def dot(a, b):
    return jnp.dot(a, b, preferred_element_type=F32)


def pair_weights(rank, pair_count, total_pairs, width):
    weights = []
    for k in range(pair_count):
        up = jnp.full((1, width), rank[2 * k], jnp.int32).astype(F32) / (2 * total_pairs - 1) - 0.5
        down = jnp.full((1, width), rank[2 * k + 1], jnp.int32).astype(F32) / (2 * total_pairs - 1) - 0.5
        weights.append((up - down).astype(BF16).astype(F32))
    return weights


def block_places(sizes, flip, r, c):
    nz, nx, ny, nc = sizes
    pop, grp = lax.axis_index("pop"), lax.axis_index("grp")
    z0, x0, y0, c0 = pop // nx, lax.rem(pop, nx), grp // nc, lax.rem(grp, nc)
    places = []
    for dx in range(nx):
        for dy in range(ny):
            for dz in range(nz):
                row = lax.rem(z0 + dz, nz) * nx + lax.rem(x0 + dx, nx)
                column = lax.rem(y0 + dy, ny) * nc + lax.rem(c0 + flip, nc)
                rows, columns = pl.ds(pl.multiple_of(row * r, r), r), pl.ds(pl.multiple_of(column * c, c), c)
                places.append(((dx, dy, dz), rows, columns))
    return places


def weighted_block(weights, held, rows, columns):
    total = None
    for k, weight in enumerate(weights):
        term = weight * held[k, rows, columns].astype(F32)
        total = term if total is None else total + term
    return total


def load_kernel(sizes, total_pairs, ranks, noise, held, sent, own, rank, sems, rank_sem):
    nz, nx, ny, nc = sizes
    pair_count = noise.shape[0]
    r, c = own.shape[3:]
    ranks_copy = pltpu.make_async_copy(ranks, rank, rank_sem)
    ranks_copy.start()
    places = [block_places(sizes, flip, r, c) for flip in range(nc)]
    copies = {}
    for (dx, dy, dz), rows, _ in places[0]:
        if dy == 0:
            here = (slice(None), rows)
            copies[dx, dz] = pltpu.make_async_copy(noise.at[here], held.at[here], sems.at[len(copies)])
            copies[dx, dz].start()
    ranks_copy.wait()
    weights = pair_weights(rank, pair_count, total_pairs, c)
    for dx in range(nx):
        for dz in range(nz):
            copies[dx, dz].wait()
            for flip in list(range(1, nc)) + [0]:
                for where, rows, columns in places[flip]:
                    if (where[0], where[2]) == (dx, dz):
                        block = weighted_block(weights, held, rows, columns)
                        if flip:
                            sent[(flip - 1,) + where] = block.astype(sent.dtype)
                        else:
                            own[where] = block


def load_noise(noise, ranks, sizes, total_pairs):
    pair_count, rows, columns = noise.shape
    nz, nx, ny, nc = sizes
    r, c = rows // (nz * nx), columns // (ny * nc)
    hbm, vmem = pl.BlockSpec(memory_space=pltpu.HBM), pl.BlockSpec(memory_space=pltpu.VMEM)
    return pl.pallas_call(
        functools.partial(load_kernel, sizes, total_pairs),
        out_shape=(
            jax.ShapeDtypeStruct(noise.shape, BF16),
            jax.ShapeDtypeStruct((nc - 1, nx, ny, nz, r, c), BF16),
            jax.ShapeDtypeStruct((nx, ny, nz, r, c), F32),
        ),
        in_specs=[hbm, hbm],
        out_specs=(vmem, vmem, vmem),
        scratch_shapes=[
            pltpu.SMEM(ranks.shape, jnp.int32),
            pltpu.SemaphoreType.DMA((nx * nz,)),
            pltpu.SemaphoreType.DMA,
        ],
        compiler_params=pltpu.CompilerParams(vmem_limit_bytes=42 * 2**20),
        cost_estimate=pl.CostEstimate(flops=10**8, bytes_accessed=2 * noise.size, transcendentals=0),
        name="load",
    )(ranks, noise)


def by_length(lengths, pair_count):
    longest = [jnp.maximum(lengths[2 * k], lengths[2 * k + 1]) for k in range(pair_count)]
    order = [jnp.int32(k) for k in range(pair_count)]
    for top in range(pair_count - 1, 0, -1):
        for k in range(top):
            swap = longest[k] < longest[k + 1]
            a, b = longest[k], longest[k + 1]
            longest[k], longest[k + 1] = jnp.where(swap, b, a), jnp.where(swap, a, b)
            a, b = order[k], order[k + 1]
            order[k], order[k + 1] = jnp.where(swap, b, a), jnp.where(swap, a, b)
    return order, longest


def rollout_kernel(begin, end, *refs):
    first_call, last_call = begin == 0, end == STEPS
    lengths, w_first, w_mid, noise = refs[:4]
    if first_call:
        start_state, w_last, dynamics, control = refs[4:8]
        rest = refs[8:]
    else:
        states_in, last_in, dynamics_in, control_in, squares_in, efforts_in = refs[4:10]
        rest = refs[10:]
    if last_call:
        returns, states, squares, efforts = rest
        last, dyn, ctl = last_in, dynamics_in, control_in
    elif first_call:
        states, last, dyn, ctl, squares, efforts = rest
    else:
        states, squares, efforts = rest
        last, dyn, ctl = last_in, dynamics_in, control_in
    pair_count, _, hidden = noise.shape
    members = 2 * pair_count
    obs = w_first.shape[0]
    batch = states.shape[0] // members
    order, longest = by_length(lengths, pair_count)
    alike = [lengths[2 * order[m // 2] + m % 2] for m in range(members)]

    def add_reward(moment, state, action, active, fresh):
        for m in range(2 * active):
            alive = jnp.where(moment < alike[m], 1.0, 0.0)
            s, a = state[m * batch : (m + 1) * batch], action[m * batch : (m + 1) * batch]
            square = alive * (s * s).reshape(batch // 8, 8, s.shape[1]).sum(axis=0)
            effort = alive * (a * a).reshape(batch // 8, 8, a.shape[1]).sum(axis=0)
            squares[m] = square if fresh else squares[m] + square
            efforts[m] = effort if fresh else efforts[m] + effort

    def finish(moment, second, moved, active, fresh):
        action = jnp.tanh(dot(second, last[...]))
        state = moved + dot(action.astype(BF16), ctl[...])
        states[: state.shape[0]] = state.astype(BF16)
        add_reward(moment, state, action, active, fresh)

    def step(active, moment, carry):
        rows = 2 * active * batch
        low = states[:rows]
        first = jnp.tanh(dot(low, w_first[...]))
        row = lax.broadcasted_iota(jnp.int32, (rows, 1), 0)
        scale = jnp.where(lax.rem(row // batch, 2) == 0, noise_scale, -noise_scale).astype(F32)
        scaled = (first * scale).astype(BF16)
        shared = dot(first.astype(BF16), w_mid[...])
        own = [dot(scaled[p * 2 * batch : (p + 1) * 2 * batch], noise[order[p]]) for p in range(active)]
        second = jnp.tanh(shared + jnp.concatenate(own, axis=0)).astype(BF16)
        finish(moment, second, dot(low, dyn[0]) + dot(low, dyn[1]), active, False)
        return carry

    def first_step():
        low = start_state[...].astype(BF16)
        first = jnp.tanh(dot(low, w_first[...]))
        scaled = (first * noise_scale).astype(BF16)
        shared = dot(first.astype(BF16), w_mid[...])
        moved = dot(low, dyn[0]) + dot(low, dyn[1])
        second = []
        for p in range(pair_count):
            own = dot(scaled, noise[order[p]])
            second += [jnp.tanh(shared + own).astype(BF16), jnp.tanh(shared - own).astype(BF16)]
        finish(0, jnp.concatenate(second, axis=0), jnp.concatenate([moved] * members, axis=0), pair_count, True)

    if first_call:
        tall = w_last[...].astype(F32).T
        last[...] = jnp.concatenate([tall, tall], axis=1).astype(BF16)
        whole = dynamics[...]
        high = whole.astype(BF16)
        dyn[0] = high
        dyn[1] = (whole - high.astype(F32)).astype(BF16)
        whole = control[...]
        high = whole.astype(BF16)
        ctl[...] = jnp.concatenate([high, (whole - high.astype(F32)).astype(BF16)], axis=0)
        first_step()
    else:
        states[...] = states_in[...]
        squares[...] = squares_in[...]
        efforts[...] = efforts_in[...]
    start = max(begin, 1)
    if end > start:
        low = start
        for active in range(pair_count, 0, -1):
            high = jnp.clip(longest[active - 1], start, end)
            lax.fori_loop(low, high, functools.partial(step, active), 0)
            low = high
    if last_call:
        acts = efforts.shape[2]
        sums = jnp.sum(squares[...].sum(axis=1), axis=1, keepdims=True) * (-1.0 / (obs * batch * STEPS))
        sums += jnp.sum(efforts[...].sum(axis=1), axis=1, keepdims=True) * (-effort_cost / (acts * batch * STEPS))
        here = lax.broadcasted_iota(jnp.int32, (members, members), 0)
        there = lax.broadcasted_iota(jnp.int32, (members, members), 1)
        place = jnp.zeros((members, members), jnp.int32)
        for m in range(members):
            place = jnp.where(here == m, 2 * order[m // 2] + m % 2, place)
        returns[...] = jnp.sum(jnp.where(place == there, sums, 0.0), axis=0)


def rollout(begin, end, lengths, w_first, w_mid, noise, others):
    pair_count, hidden, _ = noise.shape
    obs = w_first.shape[0]
    members = 2 * pair_count
    if begin == 0:
        start_state, w_last = others[:2]
        batch, acts = start_state.shape[0], w_last.shape[0]
    else:
        batch, acts = others[0].shape[0] // members, others[1].shape[1] // 2
    rows = members * batch
    sums = [((members, 8, obs), F32), ((members, 8, 2 * acts), F32)]
    weights = [((hidden, 2 * acts), BF16), ((2, obs, obs), BF16), ((2 * acts, obs), BF16)]
    kept = [((rows, obs), BF16)] + (weights if begin == 0 else []) + sums
    vmem, smem = pl.BlockSpec(memory_space=pltpu.VMEM), pl.BlockSpec(memory_space=pltpu.SMEM)
    if end == STEPS:
        out_shape = jax.ShapeDtypeStruct((members,), F32)
        out_specs = vmem
        scratch = [pltpu.VMEM(*k) for k in kept]
    else:
        out_shape = [jax.ShapeDtypeStruct(*k) for k in kept]
        out_specs = [vmem] * len(kept)
        scratch = []
    macs = (end - begin) * rows * hidden * (2 * hidden + 2 * obs)
    out = pl.pallas_call(
        functools.partial(rollout_kernel, begin, end),
        out_shape=out_shape,
        in_specs=[smem] + [vmem] * (3 + len(others)),
        out_specs=out_specs,
        scratch_shapes=scratch,
        compiler_params=pltpu.CompilerParams(vmem_limit_bytes=32 * 2**20),
        cost_estimate=pl.CostEstimate(flops=2 * macs, bytes_accessed=2 * noise.size, transcendentals=0),
        name=f"rollout_{begin}",
    )(lengths, w_first, w_mid, noise, *others)
    if begin and end < STEPS:
        out = [out[0], *others[1:4], *out[1:]]
    return out


def on_device(sizes, noise, ranks, lengths, start_state, w_first, w_mid, w_last, dynamics, control):
    nz, nx, ny, nc = sizes
    total_pairs = noise.shape[0] * nz * nx * ny * nc

    def shift(value, dz, dx, dy, dc):
        pairs = []
        for z in range(nz):
            for x in range(nx):
                for y in range(ny):
                    for c in range(nc):
                        tz, tx, ty, tc = (z + dz) % nz, (x + dx) % nx, (y + dy) % ny, (c + dc) % nc
                        pairs.append((((z * nx + x) * ny + y) * nc + c, ((tz * nx + tx) * ny + ty) * nc + tc))
        return lax.ppermute(value, ("pop", "grp"), pairs)

    noise, sent, total = load_noise(noise, ranks, sizes, total_pairs)
    for dc in range(1, nc):
        total = total + shift(sent[dc - 1], 0, 0, 0, dc).astype(F32)
    carried = rollout(CUTS[0], CUTS[1], lengths, w_first, w_mid, noise, (start_state, w_last.T, dynamics, control))
    total, carried = lax.optimization_barrier((total, carried))

    mine = total[0, 0]
    for dx in range(nx):
        for dy in range(ny):
            if dx or dy:
                mine = mine + shift(total[dx, dy].astype(BF16), 0, dx, dy, 0).astype(F32)
    carried = rollout(CUTS[1], CUTS[2], lengths, w_first, w_mid, noise, carried)
    mine, carried = lax.optimization_barrier((mine, carried))
    result = mine[0]
    for dz in range(1, nz):
        result = result + shift(mine[dz], dz, 0, 0, 0)
    returns = rollout(CUTS[2], CUTS[3], lengths, w_first, w_mid, noise, carried)
    gradient = result / (total_pairs * noise_scale)
    return (returns, gradient)


def solution(mesh):
    pop, grp = mesh.shape["pop"], mesh.shape["grp"]
    nx = max(1, pop // 4)
    nc = 2 if grp % 2 == 0 else 1
    sizes = (pop // nx, nx, grp // nc, nc)
    return jax.shard_map(
        functools.partial(on_device, sizes),
        mesh=mesh,
        in_specs=(
            P(("pop", "grp"), None, None),
            P(("pop", "grp")),
            P(("pop", "grp")),
            P(),
            P(),
            P(),
            P(),
            P(),
            P(),
        ),
        out_specs=(P(("pop", "grp")), P("pop", "grp")),
        check_vma=False,
    )
```

```python
import functools

import jax
import jax.numpy as jnp
from jax import lax
from jax.experimental import pallas as pl
from jax.experimental.pallas import tpu as pltpu
from jax.sharding import PartitionSpec as P

STEPS = 16
CUTS = (0, 1, 8, STEPS)
F32, BF16 = jnp.float32, jnp.bfloat16

noise_scale = 0.02
effort_cost = 0.1


def dot(a, b):
    return jnp.dot(a, b, preferred_element_type=F32)


def pair_weights(rank, pair_count, total_pairs, width):
    weights = []
    for k in range(pair_count):
        up = jnp.full((1, width), rank[2 * k], jnp.int32).astype(F32) / (2 * total_pairs - 1) - 0.5
        down = jnp.full((1, width), rank[2 * k + 1], jnp.int32).astype(F32) / (2 * total_pairs - 1) - 0.5
        weights.append((up - down).astype(BF16).astype(F32))
    return weights


def block_places(sizes, flip, r, c):
    nz, nx, ny, nc = sizes
    pop, grp = lax.axis_index("pop"), lax.axis_index("grp")
    z0, x0, y0, c0 = pop // nx, lax.rem(pop, nx), grp // nc, lax.rem(grp, nc)
    places = []
    for dx in range(nx):
        for dy in range(ny):
            for dz in range(nz):
                row = lax.rem(z0 + dz, nz) * nx + lax.rem(x0 + dx, nx)
                column = lax.rem(y0 + dy, ny) * nc + lax.rem(c0 + flip, nc)
                rows, columns = pl.ds(pl.multiple_of(row * r, r), r), pl.ds(pl.multiple_of(column * c, c), c)
                places.append(((dx, dy, dz), rows, columns))
    return places


def weighted_block(weights, held, rows, columns):
    total = None
    for k, weight in enumerate(weights):
        term = weight * held[k, rows, columns].astype(F32)
        total = term if total is None else total + term
    return total


def load_kernel(sizes, total_pairs, ranks, noise, held, sent, own, rank, sems, rank_sem):
    nz, nx, ny, nc = sizes
    pair_count = noise.shape[0]
    r, c = own.shape[3:]
    ranks_copy = pltpu.make_async_copy(ranks, rank, rank_sem)
    ranks_copy.start()
    places = [block_places(sizes, flip, r, c) for flip in range(nc)]
    copies = {}
    for (dx, dy, dz), rows, _ in places[0]:
        if dy == 0:
            here = (slice(None), rows)
            copies[dx, dz] = pltpu.make_async_copy(noise.at[here], held.at[here], sems.at[len(copies)])
            copies[dx, dz].start()
    ranks_copy.wait()
    weights = pair_weights(rank, pair_count, total_pairs, c)
    for dx in range(nx):
        for dz in range(nz):
            copies[dx, dz].wait()
            for flip in list(range(1, nc)) + [0]:
                for where, rows, columns in places[flip]:
                    if (where[0], where[2]) == (dx, dz):
                        block = weighted_block(weights, held, rows, columns)
                        if flip:
                            sent[(flip - 1,) + where] = block.astype(sent.dtype)
                        else:
                            own[where] = block


def load_noise(noise, ranks, sizes, total_pairs):
    pair_count, rows, columns = noise.shape
    nz, nx, ny, nc = sizes
    r, c = rows // (nz * nx), columns // (ny * nc)
    hbm, vmem = pl.BlockSpec(memory_space=pltpu.HBM), pl.BlockSpec(memory_space=pltpu.VMEM)
    return pl.pallas_call(
        functools.partial(load_kernel, sizes, total_pairs),
        out_shape=(
            jax.ShapeDtypeStruct(noise.shape, BF16),
            jax.ShapeDtypeStruct((nc - 1, nx, ny, nz, r, c), BF16),
            jax.ShapeDtypeStruct((nx, ny, nz, r, c), F32),
        ),
        in_specs=[hbm, hbm],
        out_specs=(vmem, vmem, vmem),
        scratch_shapes=[
            pltpu.SMEM(ranks.shape, jnp.int32),
            pltpu.SemaphoreType.DMA((nx * nz,)),
            pltpu.SemaphoreType.DMA,
        ],
        compiler_params=pltpu.CompilerParams(vmem_limit_bytes=24 * 2**20),
        cost_estimate=pl.CostEstimate(flops=10**8, bytes_accessed=2 * noise.size, transcendentals=0),
        name="load",
    )(*[pltpu.with_memory_space_constraint(a, pltpu.HBM) for a in (ranks, noise)])


def by_length(lengths, pair_count):
    longest = [jnp.maximum(lengths[2 * k], lengths[2 * k + 1]) for k in range(pair_count)]
    order = [jnp.int32(k) for k in range(pair_count)]
    for top in range(pair_count - 1, 0, -1):
        for k in range(top):
            swap = longest[k] < longest[k + 1]
            a, b = longest[k], longest[k + 1]
            longest[k], longest[k + 1] = jnp.where(swap, b, a), jnp.where(swap, a, b)
            a, b = order[k], order[k + 1]
            order[k], order[k + 1] = jnp.where(swap, b, a), jnp.where(swap, a, b)
    return order, longest


def rollout_kernel(begin, end, *refs):
    first_call, last_call = begin == 0, end == STEPS
    lengths, w_first, w_mid, noise = refs[:4]
    if first_call:
        start_state, w_last, dynamics, control = refs[4:8]
        rest = refs[8:]
    else:
        states_in, last_in, dynamics_in, control_in, squares_in, efforts_in = refs[4:10]
        rest = refs[10:]
    if last_call:
        returns, states, squares, efforts = rest
        last, dyn, ctl = last_in, dynamics_in, control_in
    elif first_call:
        states, last, dyn, ctl, squares, efforts = rest
    else:
        states, squares, efforts = rest
        last, dyn, ctl = last_in, dynamics_in, control_in
    pair_count, _, hidden = noise.shape
    members = 2 * pair_count
    obs = w_first.shape[0]
    batch = states.shape[0] // members
    order, longest = by_length(lengths, pair_count)
    alike = [lengths[2 * order[m // 2] + m % 2] for m in range(members)]

    def add_reward(moment, state, action, active, fresh):
        for m in range(2 * active):
            alive = jnp.where(moment < alike[m], 1.0, 0.0)
            s, a = state[m * batch : (m + 1) * batch], action[m * batch : (m + 1) * batch]
            square = alive * (s * s).reshape(batch // 8, 8, s.shape[1]).sum(axis=0)
            effort = alive * (a * a).reshape(batch // 8, 8, a.shape[1]).sum(axis=0)
            squares[m] = square if fresh else squares[m] + square
            efforts[m] = effort if fresh else efforts[m] + effort

    def finish(moment, second, moved, active, fresh):
        action = jnp.tanh(dot(second, last[...]))
        state = moved + dot(action.astype(BF16), ctl[...])
        states[: state.shape[0]] = state.astype(BF16)
        add_reward(moment, state, action, active, fresh)

    def step(active, moment, carry):
        rows = 2 * active * batch
        low = states[:rows]
        first = jnp.tanh(dot(low, w_first[...]))
        row = lax.broadcasted_iota(jnp.int32, (rows, 1), 0)
        scale = jnp.where(lax.rem(row // batch, 2) == 0, noise_scale, -noise_scale).astype(F32)
        scaled = (first * scale).astype(BF16)
        shared = dot(first.astype(BF16), w_mid[...])
        own = [dot(scaled[p * 2 * batch : (p + 1) * 2 * batch], noise[order[p]]) for p in range(active)]
        second = jnp.tanh(shared + jnp.concatenate(own, axis=0)).astype(BF16)
        finish(moment, second, dot(low, dyn[0]) + dot(low, dyn[1]), active, False)
        return carry

    def first_step():
        low = start_state[...].astype(BF16)
        first = jnp.tanh(dot(low, w_first[...]))
        scaled = (first * noise_scale).astype(BF16)
        shared = dot(first.astype(BF16), w_mid[...])
        moved = dot(low, dyn[0]) + dot(low, dyn[1])
        second = []
        for p in range(pair_count):
            own = dot(scaled, noise[order[p]])
            second += [jnp.tanh(shared + own).astype(BF16), jnp.tanh(shared - own).astype(BF16)]
        finish(0, jnp.concatenate(second, axis=0), jnp.concatenate([moved] * members, axis=0), pair_count, True)

    if first_call:
        tall = w_last[...].astype(F32).T
        last[...] = jnp.concatenate([tall, tall], axis=1).astype(BF16)
        whole = dynamics[...]
        high = whole.astype(BF16)
        dyn[0] = high
        dyn[1] = (whole - high.astype(F32)).astype(BF16)
        whole = control[...]
        high = whole.astype(BF16)
        ctl[...] = jnp.concatenate([high, (whole - high.astype(F32)).astype(BF16)], axis=0)
        first_step()
    else:
        states[...] = states_in[...]
        squares[...] = squares_in[...]
        efforts[...] = efforts_in[...]
    start = max(begin, 1)
    if end > start:
        low = start
        for active in range(pair_count, 0, -1):
            high = jnp.clip(longest[active - 1], start, end)
            lax.fori_loop(low, high, functools.partial(step, active), 0)
            low = high
    if last_call:
        acts = efforts.shape[2]
        sums = jnp.sum(squares[...].sum(axis=1), axis=1, keepdims=True) * (-1.0 / (obs * batch * STEPS))
        sums += jnp.sum(efforts[...].sum(axis=1), axis=1, keepdims=True) * (-effort_cost / (acts * batch * STEPS))
        here = lax.broadcasted_iota(jnp.int32, (members, members), 0)
        there = lax.broadcasted_iota(jnp.int32, (members, members), 1)
        place = jnp.zeros((members, members), jnp.int32)
        for m in range(members):
            place = jnp.where(here == m, 2 * order[m // 2] + m % 2, place)
        returns[...] = jnp.sum(jnp.where(place == there, sums, 0.0), axis=0)


def rollout(begin, end, lengths, w_first, w_mid, noise, others):
    pair_count, hidden, _ = noise.shape
    obs = w_first.shape[0]
    members = 2 * pair_count
    if begin == 0:
        start_state, w_last = others[:2]
        batch, acts = start_state.shape[0], w_last.shape[0]
    else:
        batch, acts = others[0].shape[0] // members, others[1].shape[1] // 2
    rows = members * batch
    sums = [((members, 8, obs), F32), ((members, 8, 2 * acts), F32)]
    weights = [((hidden, 2 * acts), BF16), ((2, obs, obs), BF16), ((2 * acts, obs), BF16)]
    kept = [((rows, obs), BF16)] + (weights if begin == 0 else []) + sums
    vmem, smem = pl.BlockSpec(memory_space=pltpu.VMEM), pl.BlockSpec(memory_space=pltpu.SMEM)
    if end == STEPS:
        out_shape = jax.ShapeDtypeStruct((members,), F32)
        out_specs = vmem
        scratch = [pltpu.VMEM(*k) for k in kept]
    else:
        out_shape = [jax.ShapeDtypeStruct(*k) for k in kept]
        out_specs = [vmem] * len(kept)
        scratch = []
    macs = (end - begin) * rows * hidden * (2 * hidden + 2 * obs)
    out = pl.pallas_call(
        functools.partial(rollout_kernel, begin, end),
        out_shape=out_shape,
        in_specs=[smem] + [vmem] * (3 + len(others)),
        out_specs=out_specs,
        scratch_shapes=scratch,
        compiler_params=pltpu.CompilerParams(vmem_limit_bytes=32 * 2**20),
        cost_estimate=pl.CostEstimate(flops=2 * macs, bytes_accessed=2 * noise.size, transcendentals=0),
        name=f"rollout_{begin}",
    )(lengths, w_first, w_mid, noise, *others)
    if begin and end < STEPS:
        out = [out[0], *others[1:4], *out[1:]]
    return out


def on_device(sizes, noise, ranks, lengths, start_state, w_first, w_mid, w_last, dynamics, control):
    nz, nx, ny, nc = sizes
    total_pairs = noise.shape[0] * nz * nx * ny * nc

    def shift(value, dz, dx, dy, dc):
        pairs = []
        for z in range(nz):
            for x in range(nx):
                for y in range(ny):
                    for c in range(nc):
                        tz, tx, ty, tc = (z + dz) % nz, (x + dx) % nx, (y + dy) % ny, (c + dc) % nc
                        pairs.append((((z * nx + x) * ny + y) * nc + c, ((tz * nx + tx) * ny + ty) * nc + tc))
        return lax.ppermute(value, ("pop", "grp"), pairs)

    noise, sent, total = load_noise(noise, ranks, sizes, total_pairs)
    for dc in range(1, nc):
        total = total + shift(sent[dc - 1], 0, 0, 0, dc).astype(F32)
    carried = rollout(CUTS[0], CUTS[1], lengths, w_first, w_mid, noise, (start_state, w_last.T, dynamics, control))
    total, carried = lax.optimization_barrier((total, carried))

    mine = total[0, 0]
    for dx in range(nx):
        for dy in range(ny):
            if dx or dy:
                mine = mine + shift(total[dx, dy].astype(BF16), 0, dx, dy, 0).astype(F32)
    carried = rollout(CUTS[1], CUTS[2], lengths, w_first, w_mid, noise, carried)
    mine, carried = lax.optimization_barrier((mine, carried))
    result = mine[0]
    for dz in range(1, nz):
        result = result + shift(mine[dz], dz, 0, 0, 0)
    returns = rollout(CUTS[2], CUTS[3], lengths, w_first, w_mid, noise, carried)
    gradient = result / (total_pairs * noise_scale)
    return (returns, gradient)


def solution(mesh):
    pop, grp = mesh.shape["pop"], mesh.shape["grp"]
    nx = max(1, pop // 4)
    nc = 2 if grp % 2 == 0 else 1
    sizes = (pop // nx, nx, grp // nc, nc)
    return jax.shard_map(
        functools.partial(on_device, sizes),
        mesh=mesh,
        in_specs=(
            P(("pop", "grp"), None, None),
            P(("pop", "grp")),
            P(("pop", "grp")),
            P(),
            P(),
            P(),
            P(),
            P(),
            P(),
        ),
        out_specs=(P(("pop", "grp")), P("pop", "grp")),
        check_vma=False,
    )
```

```python
import functools

import jax
import jax.numpy as jnp
from jax import lax
from jax.experimental import pallas as pl
from jax.experimental.pallas import tpu as pltpu
from jax.sharding import PartitionSpec as P

STEPS = 16
CUTS = (0, 1, 8, STEPS)
F32, BF16 = jnp.float32, jnp.bfloat16

noise_scale = 0.02
effort_cost = 0.1


def dot(a, b):
    return jnp.dot(a, b, preferred_element_type=F32)


def pair_weights(rank, pair_count, total_pairs, width):
    weights = []
    for k in range(pair_count):
        up = jnp.full((1, width), rank[2 * k], jnp.int32).astype(F32) / (2 * total_pairs - 1) - 0.5
        down = jnp.full((1, width), rank[2 * k + 1], jnp.int32).astype(F32) / (2 * total_pairs - 1) - 0.5
        weights.append((up - down).astype(BF16).astype(F32))
    return weights


def block_places(sizes, flip, r, c):
    nz, nx, ny, nc = sizes
    pop, grp = lax.axis_index("pop"), lax.axis_index("grp")
    z0, x0, y0, c0 = pop // nx, lax.rem(pop, nx), grp // nc, lax.rem(grp, nc)
    places = []
    for dx in range(nx):
        for dy in range(ny):
            for dz in range(nz):
                row = lax.rem(z0 + dz, nz) * nx + lax.rem(x0 + dx, nx)
                column = lax.rem(y0 + dy, ny) * nc + lax.rem(c0 + flip, nc)
                rows, columns = pl.ds(pl.multiple_of(row * r, r), r), pl.ds(pl.multiple_of(column * c, c), c)
                places.append(((dx, dy, dz), rows, columns))
    return places


def weighted_block(weights, held, rows, columns):
    total = None
    for k, weight in enumerate(weights):
        term = weight * held[k, rows, columns].astype(F32)
        total = term if total is None else total + term
    return total


def load_kernel(sizes, total_pairs, ranks, noise, held, sent, own, rank, sems, rank_sem):
    nz, nx, ny, nc = sizes
    pair_count = noise.shape[0]
    r, c = own.shape[3:]
    ranks_copy = pltpu.make_async_copy(ranks, rank, rank_sem)
    ranks_copy.start()
    places = [block_places(sizes, flip, r, c) for flip in range(nc)]
    copies = {}
    for (dx, dy, dz), rows, _ in places[0]:
        if dy == 0:
            here = (slice(None), rows)
            copies[dx, dz] = pltpu.make_async_copy(noise.at[here], held.at[here], sems.at[len(copies)])
            copies[dx, dz].start()
    ranks_copy.wait()
    weights = pair_weights(rank, pair_count, total_pairs, c)
    for dx in range(nx):
        for dz in range(nz):
            copies[dx, dz].wait()
            for flip in list(range(1, nc)) + [0]:
                for where, rows, columns in places[flip]:
                    if (where[0], where[2]) == (dx, dz):
                        block = weighted_block(weights, held, rows, columns)
                        if flip:
                            sent[(flip - 1,) + where] = block.astype(sent.dtype)
                        else:
                            own[where] = block


def load_noise(noise, ranks, sizes, total_pairs):
    pair_count, rows, columns = noise.shape
    nz, nx, ny, nc = sizes
    r, c = rows // (nz * nx), columns // (ny * nc)
    hbm, vmem = pl.BlockSpec(memory_space=pltpu.HBM), pl.BlockSpec(memory_space=pltpu.VMEM)
    return pl.pallas_call(
        functools.partial(load_kernel, sizes, total_pairs),
        out_shape=(
            jax.ShapeDtypeStruct(noise.shape, BF16),
            jax.ShapeDtypeStruct((nc - 1, nx, ny, nz, r, c), BF16),
            jax.ShapeDtypeStruct((nx, ny, nz, r, c), F32),
        ),
        in_specs=[hbm, hbm],
        out_specs=(vmem, vmem, vmem),
        scratch_shapes=[
            pltpu.SMEM(ranks.shape, jnp.int32),
            pltpu.SemaphoreType.DMA((nx * nz,)),
            pltpu.SemaphoreType.DMA,
        ],
        compiler_params=pltpu.CompilerParams(vmem_limit_bytes=24 * 2**20),
        cost_estimate=pl.CostEstimate(flops=10**8, bytes_accessed=2 * noise.size, transcendentals=0),
        name="load",
    )(*[pltpu.with_memory_space_constraint(a, pltpu.HBM) for a in (ranks, noise)])


def by_length(lengths, pair_count):
    longest = [jnp.maximum(lengths[2 * k], lengths[2 * k + 1]) for k in range(pair_count)]
    order = [jnp.int32(k) for k in range(pair_count)]
    for top in range(pair_count - 1, 0, -1):
        for k in range(top):
            swap = longest[k] < longest[k + 1]
            a, b = longest[k], longest[k + 1]
            longest[k], longest[k + 1] = jnp.where(swap, b, a), jnp.where(swap, a, b)
            a, b = order[k], order[k + 1]
            order[k], order[k + 1] = jnp.where(swap, b, a), jnp.where(swap, a, b)
    return order, longest


def rollout_kernel(begin, end, *refs):
    first_call, last_call = begin == 0, end == STEPS
    lengths, w_first, w_mid, noise = refs[:4]
    if first_call:
        start_state, w_last, dynamics, control = refs[4:8]
        rest = refs[8:]
    else:
        states_in, last_in, dynamics_in, control_in, squares_in, efforts_in = refs[4:10]
        rest = refs[10:]
    if last_call:
        returns, states, squares, efforts = rest
        last, dyn, ctl = last_in, dynamics_in, control_in
    elif first_call:
        states, last, dyn, ctl, squares, efforts = rest
    else:
        states, squares, efforts = rest
        last, dyn, ctl = last_in, dynamics_in, control_in
    pair_count, _, hidden = noise.shape
    members = 2 * pair_count
    obs = w_first.shape[0]
    batch = states.shape[0] // members
    order, longest = by_length(lengths, pair_count)
    alike = [lengths[2 * order[m // 2] + m % 2] for m in range(members)]

    def add_reward(moment, state, action, active, fresh):
        for m in range(2 * active):
            alive = jnp.where(moment < alike[m], 1.0, 0.0)
            s, a = state[m * batch : (m + 1) * batch], action[m * batch : (m + 1) * batch]
            square = alive * (s * s).reshape(batch // 8, 8, s.shape[1]).sum(axis=0)
            effort = alive * (a * a).reshape(batch // 8, 8, a.shape[1]).sum(axis=0)
            squares[m] = square if fresh else squares[m] + square
            efforts[m] = effort if fresh else efforts[m] + effort

    def finish(moment, second, moved, active, fresh):
        action = jnp.tanh(dot(second, last[...]))
        state = moved + dot(action.astype(BF16), ctl[...])
        states[: state.shape[0]] = state.astype(BF16)
        add_reward(moment, state, action, active, fresh)

    def step(active, moment, carry):
        rows = 2 * active * batch
        low = states[:rows]
        first = jnp.tanh(dot(low, w_first[...]))
        row = lax.broadcasted_iota(jnp.int32, (rows, 1), 0)
        scale = jnp.where(lax.rem(row // batch, 2) == 0, noise_scale, -noise_scale).astype(F32)
        scaled = (first * scale).astype(BF16)
        shared = dot(first.astype(BF16), w_mid[...])
        own = [dot(scaled[p * 2 * batch : (p + 1) * 2 * batch], noise[order[p]]) for p in range(active)]
        second = jnp.tanh(shared + jnp.concatenate(own, axis=0)).astype(BF16)
        finish(moment, second, dot(low, dyn[0]) + dot(low, dyn[1]), active, False)
        return carry

    def first_step():
        low = start_state[...].astype(BF16)
        first = jnp.tanh(dot(low, w_first[...]))
        scaled = (first * noise_scale).astype(BF16)
        shared = dot(first.astype(BF16), w_mid[...])
        moved = dot(low, dyn[0]) + dot(low, dyn[1])
        second = []
        for p in range(pair_count):
            own = dot(scaled, noise[order[p]])
            second += [jnp.tanh(shared + own).astype(BF16), jnp.tanh(shared - own).astype(BF16)]
        finish(0, jnp.concatenate(second, axis=0), jnp.concatenate([moved] * members, axis=0), pair_count, True)

    if first_call:
        tall = w_last[...].astype(F32).T
        last[...] = jnp.concatenate([tall, tall], axis=1).astype(BF16)
        whole = dynamics[...]
        high = whole.astype(BF16)
        dyn[0] = high
        dyn[1] = (whole - high.astype(F32)).astype(BF16)
        whole = control[...]
        high = whole.astype(BF16)
        ctl[...] = jnp.concatenate([high, (whole - high.astype(F32)).astype(BF16)], axis=0)
        first_step()
    else:
        states[...] = states_in[...]
        squares[...] = squares_in[...]
        efforts[...] = efforts_in[...]
    start = max(begin, 1)
    if end > start:
        low = start
        for active in range(pair_count, 0, -1) if last_call else (pair_count,):
            high = jnp.clip(longest[active - 1], start, end) if last_call else end
            lax.fori_loop(low, high, functools.partial(step, active), 0)
            low = high
    if last_call:
        acts = efforts.shape[2]
        sums = jnp.sum(squares[...].sum(axis=1), axis=1, keepdims=True) * (-1.0 / (obs * batch * STEPS))
        sums += jnp.sum(efforts[...].sum(axis=1), axis=1, keepdims=True) * (-effort_cost / (acts * batch * STEPS))
        here = lax.broadcasted_iota(jnp.int32, (members, members), 0)
        there = lax.broadcasted_iota(jnp.int32, (members, members), 1)
        place = jnp.zeros((members, members), jnp.int32)
        for m in range(members):
            place = jnp.where(here == m, 2 * order[m // 2] + m % 2, place)
        returns[...] = jnp.sum(jnp.where(place == there, sums, 0.0), axis=0)


def rollout(begin, end, lengths, w_first, w_mid, noise, others):
    pair_count, hidden, _ = noise.shape
    obs = w_first.shape[0]
    members = 2 * pair_count
    if begin == 0:
        start_state, w_last = others[:2]
        batch, acts = start_state.shape[0], w_last.shape[0]
    else:
        batch, acts = others[0].shape[0] // members, others[1].shape[1] // 2
    rows = members * batch
    sums = [((members, 8, obs), F32), ((members, 8, 2 * acts), F32)]
    weights = [((hidden, 2 * acts), BF16), ((2, obs, obs), BF16), ((2 * acts, obs), BF16)]
    kept = [((rows, obs), BF16)] + (weights if begin == 0 else []) + sums
    vmem, smem = pl.BlockSpec(memory_space=pltpu.VMEM), pl.BlockSpec(memory_space=pltpu.SMEM)
    if end == STEPS:
        out_shape = jax.ShapeDtypeStruct((members,), F32)
        out_specs = vmem
        scratch = [pltpu.VMEM(*k) for k in kept]
    else:
        out_shape = [jax.ShapeDtypeStruct(*k) for k in kept]
        out_specs = [vmem] * len(kept)
        scratch = []
    macs = (end - begin) * rows * hidden * (2 * hidden + 2 * obs)
    out = pl.pallas_call(
        functools.partial(rollout_kernel, begin, end),
        out_shape=out_shape,
        in_specs=[smem] + [vmem] * (3 + len(others)),
        out_specs=out_specs,
        scratch_shapes=scratch,
        compiler_params=pltpu.CompilerParams(vmem_limit_bytes=32 * 2**20),
        cost_estimate=pl.CostEstimate(flops=2 * macs, bytes_accessed=2 * noise.size, transcendentals=0),
        name=f"rollout_{begin}",
    )(lengths, w_first, w_mid, noise, *others)
    if begin and end < STEPS:
        out = [out[0], *others[1:4], *out[1:]]
    return out


def on_device(sizes, noise, ranks, lengths, start_state, w_first, w_mid, w_last, dynamics, control):
    nz, nx, ny, nc = sizes
    total_pairs = noise.shape[0] * nz * nx * ny * nc

    def shift(value, dz, dx, dy, dc):
        pairs = []
        for z in range(nz):
            for x in range(nx):
                for y in range(ny):
                    for c in range(nc):
                        tz, tx, ty, tc = (z + dz) % nz, (x + dx) % nx, (y + dy) % ny, (c + dc) % nc
                        pairs.append((((z * nx + x) * ny + y) * nc + c, ((tz * nx + tx) * ny + ty) * nc + tc))
        return lax.ppermute(value, ("pop", "grp"), pairs)

    noise, sent, total = load_noise(noise, ranks, sizes, total_pairs)
    for dc in range(1, nc):
        total = total + shift(sent[dc - 1], 0, 0, 0, dc).astype(F32)
    carried = rollout(CUTS[0], CUTS[1], lengths, w_first, w_mid, noise, (start_state, w_last.T, dynamics, control))
    total, carried = lax.optimization_barrier((total, carried))

    mine = total[0, 0]
    for dx in range(nx):
        for dy in range(ny):
            if dx or dy:
                mine = mine + shift(total[dx, dy].astype(BF16), 0, dx, dy, 0).astype(F32)
    carried = rollout(CUTS[1], CUTS[2], lengths, w_first, w_mid, noise, carried)
    mine, carried = lax.optimization_barrier((mine, carried))
    result = mine[0]
    for dz in range(1, nz):
        result = result + shift(mine[dz], dz, 0, 0, 0)
    returns = rollout(CUTS[2], CUTS[3], lengths, w_first, w_mid, noise, carried)
    gradient = result / (total_pairs * noise_scale)
    return (returns, gradient)


def solution(mesh):
    pop, grp = mesh.shape["pop"], mesh.shape["grp"]
    nx = max(1, pop // 4)
    nc = 2 if grp % 2 == 0 else 1
    sizes = (pop // nx, nx, grp // nc, nc)
    return jax.shard_map(
        functools.partial(on_device, sizes),
        mesh=mesh,
        in_specs=(
            P(("pop", "grp"), None, None),
            P(("pop", "grp")),
            P(("pop", "grp")),
            P(),
            P(),
            P(),
            P(),
            P(),
            P(),
        ),
        out_specs=(P(("pop", "grp")), P("pop", "grp")),
        check_vma=False,
    )
```
